32 devices in a mesh: expert: 4 (over z), shard: 8 (over y, x, core).
Axes of the slice: x: 2, y: 2, z: 4, core: 2. Of those that a mesh axis runs over, the one named last changes fastest.
Arguments:
- master_gate: float32 [64, 2048, 1408], P('expert', 'shard'), may hold values from -0.1875 to 0.1875
- master_up: float32 [64, 2048, 1408], P('expert', 'shard'), may hold values from -0.1875 to 0.1875
- router_weight: float32 [2048, 64], P('shard', 'expert'), may hold values from -0.125 to 0.125
- router_gain: float32 [2048], P('shard'), may hold values from 0.25 to 1.75
Outputs:
- final_gate: bfloat16 [64, 2048, 1408], P('expert', None, 'shard')
- final_up: bfloat16 [64, 2048, 1408], P('expert', None, 'shard')
- scale_gate: float32 [64, 1408], P('expert', 'shard')
- scale_up: float32 [64, 1408], P('expert', 'shard')
- serve_router: bfloat16 [2048, 64], replicated
The draws below stay inside these ranges and needn't reach their ends.
All inputs are finite; a program needn't handle non-finite values.
Results may differ from the reference program's by a relative error of at most 0.001.
Values may be sent and summed in bfloat16 or wider, within the bound.
A program may use at most 192 MiB of HBM per device.

```python
import jax
import jax.numpy as jnp
from jax import lax

EXPERTS = 64
D_MODEL = 2048
D_EXPERT = 1408


def strengthened(entries, stream_key, source, target, blocks, factor):
    def block_of(position):
        return (jnp.arange(entries.shape[position]) // (entries.shape[position] // blocks)).reshape((-1,) + (1,) * (entries.ndim - 1 - position))

    one_side = jax.random.permutation(stream_key, blocks)[block_of(target)]
    second = (block_of(target) + blocks // 2) % blocks
    return jnp.where((block_of(source) == one_side) | (block_of(source) == second), factor * entries, entries)


def block_levels(key, dims, pieces, least, top_value):
    def one(position, shards_of):
        heights = jax.random.uniform(jax.random.fold_in(jax.random.fold_in(key, 6), position), (shards_of,), jnp.float32, least / len(pieces), top_value / len(pieces))
        return jnp.repeat(jnp.exp(heights), dims[position] // shards_of).reshape((-1,) + (1,) * (len(dims) - position - 1))

    level = one(*pieces[0])
    for cut in pieces[1:]:
        level = level * one(*cut)
    return level


def bell_draw(own_key, extent, deviation, limit, pieces=(), held_as=jnp.bfloat16):
    result = deviation * jax.random.normal(own_key, extent, jnp.float32)
    if pieces:
        result = result * block_levels(own_key, extent, pieces, -0.22, 0.18)
    return jnp.clip(result, -limit, limit).astype(held_as)


def gaussian_with(rng, shape, width, bound, pieces, heavy, kind=jnp.bfloat16):
    entries = width * jax.random.normal(rng, shape, jnp.float32)
    if pieces:
        entries = entries * block_levels(rng, shape, pieces, -0.22, 0.18)
    return jnp.clip(strengthened(entries, jax.random.fold_in(rng, 3), *heavy), -bound, bound).astype(kind)


def setup_inputs(seed: int = 0) -> dict:
    seeds = jax.random.split(jax.random.key(seed), 5)
    master_gate = gaussian_with(seeds[0], (EXPERTS, D_MODEL, D_EXPERT), D_MODEL ** -0.5, 0.1875, ((0, 4), (1, 8)), (1, 2, 8, 2.0), jnp.float32)
    master_up = gaussian_with(seeds[1], (EXPERTS, D_MODEL, D_EXPERT), D_MODEL ** -0.5, 0.1875, ((0, 4), (1, 8)), (1, 2, 8, 2.0), jnp.float32)
    router_weight = bell_draw(seeds[2], (D_MODEL, EXPERTS), D_MODEL ** -0.5, 0.125, ((0, 8), (1, 4)), jnp.float32)
    router_gain = jnp.clip(1.0 + 0.15 * jax.random.normal(seeds[3], (D_MODEL,), jnp.float32), 0.25, 1.75)
    return dict(master_gate=master_gate, master_up=master_up, router_weight=router_weight, router_gain=router_gain)


def reference(master_gate, master_up, router_weight, router_gain):
    scale_gate = jnp.sqrt(lax.optimization_barrier(jnp.sum(master_gate * master_gate, axis=1)))
    final_gate = (master_gate / jnp.expand_dims(scale_gate, 1)).astype(jnp.bfloat16)
    scale_up = jnp.sqrt(lax.optimization_barrier(jnp.sum(master_up * master_up, axis=1)))
    final_up = (master_up / jnp.expand_dims(scale_up, 1)).astype(jnp.bfloat16)
    serve_router = (router_weight * router_gain[:, None]).astype(jnp.bfloat16)
    return (final_gate, final_up, scale_gate, scale_up, serve_router)
```

```python
import functools

import jax
import jax.numpy as jnp
from jax import lax
from jax.experimental import pallas as pl
from jax.experimental.pallas import tpu as pltpu
from jax.sharding import PartitionSpec as P

GROUP = 8
SLOTS = 16
LANES = 128
VMEM_LIMIT = 62914560


def plain(master_gate, master_up, router_weight, router_gain):
    total_gate, total_up = lax.psum(
        (jnp.sum(master_gate * master_gate, axis=1), jnp.sum(master_up * master_up, axis=1)),
        "shard",
    )
    scale_gate = jnp.sqrt(total_gate)
    scale_up = jnp.sqrt(total_up)
    narrow_gate, narrow_up = (
        (master_gate / jnp.expand_dims(scale_gate, 1)).astype(jnp.bfloat16),
        (master_up / jnp.expand_dims(scale_up, 1)).astype(jnp.bfloat16),
    )
    final_gate, final_up = (
        lax.all_to_all(narrow_gate, "shard", split_axis=2, concat_axis=1, tiled=True),
        lax.all_to_all(narrow_up, "shard", split_axis=2, concat_axis=1, tiled=True),
    )
    scale_gate = lax.dynamic_slice_in_dim(
        scale_gate, lax.axis_index("shard") * final_gate.shape[2], final_gate.shape[2], axis=1
    )
    scale_up = lax.dynamic_slice_in_dim(
        scale_up, lax.axis_index("shard") * final_up.shape[2], final_up.shape[2], axis=1
    )
    part_router = (router_weight * router_gain[:, None]).astype(jnp.bfloat16)
    row_router = lax.all_gather(part_router, "shard", axis=0, tiled=True)
    serve_router = lax.all_gather(row_router, "expert", axis=1, tiled=True)
    return (final_gate, final_up, scale_gate, scale_up, serve_router)


def kernel(n, nz, gate, up, weight, gain, out, scale_out, router_out,
           buf, slots, part, got, inverse, column,
           load_sem, send_sem, own_sem, recv_sem, part_send, part_recv,
           first_send, first_recv, second_send, second_recv, router_own):
    me = lax.axis_index("shard")
    mez = lax.axis_index("expert")
    experts, rows, width = gate.shape
    slabs = 2 * experts
    groups = slabs // GROUP
    narrow = width // n
    router_rows = weight.shape[0]

    def load(source, e, k):
        return pltpu.make_async_copy(source.at[e], buf.at[k], load_sem.at[k])

    def start_gate(e, _):
        load(gate, e, e).start()
        return 0

    def start_up(e, _):
        load(up, e, experts + e).start()
        return 0

    lax.fori_loop(0, experts, start_gate, 0)
    lax.fori_loop(0, experts, start_up, 0)

    barrier = pltpu.get_barrier_semaphore()
    for r in range(1, n):
        pl.semaphore_signal(barrier, inc=1, device_id={"shard": lax.rem(me + r, n)},
                            device_id_type=pl.DeviceIdType.MESH)
    for r in range(1, nz):
        pl.semaphore_signal(barrier, inc=1, device_id={"expert": lax.rem(mez + r, nz)},
                            device_id_type=pl.DeviceIdType.MESH)

    my_rows = pl.ds(pl.multiple_of(mez * router_rows, router_rows), router_rows)
    my_lanes = pl.ds(pl.multiple_of(me * rows, rows), rows)
    column[my_rows, :] = (weight[...] * gain[...]).astype(jnp.bfloat16)
    pl.semaphore_wait(barrier, n - 1 + nz - 1)

    def sums(g):
        def one(i, _):
            k = g * GROUP + i
            load(gate, 0, k).wait()
            x = buf[k]
            part[g, pl.ds(i, 1), :] = jnp.sum(x * x, axis=0, keepdims=True)
            return 0
        lax.fori_loop(0, GROUP, one, 0)

    def part_copy(g, r):
        return pltpu.make_async_remote_copy(
            src_ref=part.at[g], dst_ref=got.at[g, r - 1],
            send_sem=part_send.at[g, r - 1], recv_sem=part_recv.at[g, r - 1],
            device_id={"shard": lax.rem(me + r, n)}, device_id_type=pl.DeviceIdType.MESH)

    def send_part(g):
        for r in range(1, n):
            part_copy(g, r).start()

    def first_copy(r):
        return pltpu.make_async_remote_copy(
            src_ref=column.at[my_rows, :], dst_ref=column.at[my_rows, :],
            send_sem=first_send.at[r - 1], recv_sem=first_recv.at[r - 1],
            device_id={"expert": lax.rem(mez + r, nz)}, device_id_type=pl.DeviceIdType.MESH)

    def second_copy(r):
        return pltpu.make_async_remote_copy(
            src_ref=column, dst_ref=router_out.at[:, my_lanes],
            send_sem=second_send.at[r - 1], recv_sem=second_recv.at[r - 1],
            device_id={"shard": lax.rem(me + r, n)}, device_id_type=pl.DeviceIdType.MESH)

    own_router = pltpu.make_async_copy(column, router_out.at[:, my_lanes], router_own)

    def slab_copy(k, r):
        target = lax.rem(me + r, n)
        s = k % SLOTS
        return pltpu.make_async_remote_copy(
            src_ref=slots.at[s, pl.ds(pl.multiple_of(target * narrow, 16), narrow), :],
            dst_ref=out.at[k, :, my_lanes],
            send_sem=send_sem.at[s, r - 1], recv_sem=recv_sem.at[r - 1],
            device_id={"shard": target}, device_id_type=pl.DeviceIdType.MESH)

    def own_copy(k):
        s = k % SLOTS
        return pltpu.make_async_copy(
            slots.at[s, pl.ds(pl.multiple_of(me * narrow, 16), narrow), :],
            out.at[k, :, my_lanes], own_sem.at[s])

    def send_slab(k):
        for r in range(1, n):
            slab_copy(k, r).start()
        own_copy(k).start()

    def wait_slab(k):
        for r in range(1, n):
            slab_copy(k, r).wait_send()
        own_copy(k).wait()

    def narrow_slab(g, i):
        k = g * GROUP + i

        @pl.when(k >= SLOTS)
        def _():
            wait_slab(k - SLOTS)

        s = k % SLOTS

        def tile(j, _):
            lanes = pl.ds(pl.multiple_of(j * LANES, LANES), LANES)
            y = buf[k, :, lanes] * inverse[j, pl.ds(k, 1), :]
            slots[s, lanes, :] = y.T.astype(jnp.bfloat16)
            return 0

        lax.fori_loop(0, width // LANES, tile, 0)

    for g in range(groups):
        sums(g)
        if g == 0:
            for r in range(1, nz):
                first_copy(r).start()
        else:
            send_part(g - 1)
        if g == 1:
            for r in range(1, nz):
                first_copy(r).wait()
            for r in range(1, n):
                second_copy(r).start()
            own_router.start()

    for g in range(groups):
        for r in range(1, n):
            part_copy(g, r).wait_recv()
        total = part[g]
        for r in range(1, n):
            total = total + got[g, r - 1]
        scale = jnp.sqrt(total)
        scale_out[g * GROUP:(g + 1) * GROUP, :] = scale
        reciprocal = 1.0 / scale
        for j in range(width // LANES):
            inverse[j, g * GROUP:(g + 1) * GROUP, :] = reciprocal[:, j * LANES:(j + 1) * LANES]

        def step(i, _):
            narrow_slab(g, i)
            k = g * GROUP + i

            @pl.when(k > 0)
            def _():
                send_slab(k - 1)

            if g == 0:
                @pl.when(k == 0)
                def _():
                    send_part(groups - 1)
            return 0

        lax.fori_loop(0, GROUP, step, 0)

    for r in range(1, n):
        second_copy(r).wait_send()
    for g in range(groups):
        for r in range(1, n):
            part_copy(g, r).wait_send()
    send_slab(slabs - 1)

    def drain(k, _):
        wait_slab(k)
        return 0

    lax.fori_loop(max(slabs - SLOTS, 0), slabs, drain, 0)
    own_router.wait()
    for r in range(1, n):
        second_copy(r).wait_recv()
        whole = out.at[:, :, my_lanes]
        pltpu.make_async_remote_copy(
            src_ref=whole, dst_ref=whole,
            send_sem=send_sem.at[0, r - 1], recv_sem=recv_sem.at[r - 1],
            device_id={"shard": lax.rem(me + r, n)}, device_id_type=pl.DeviceIdType.MESH,
        ).wait_recv()


def fused(n, nz, master_gate, master_up, router_weight, router_gain):
    experts, rows, width = master_gate.shape
    slabs = 2 * experts
    groups = slabs // GROUP
    narrow = width // n
    router_rows = router_weight.shape[1]
    hbm = pl.BlockSpec(memory_space=pl.ANY)
    vmem = pl.BlockSpec(memory_space=pltpu.VMEM)
    dma = pltpu.SemaphoreType.DMA
    out, scale, router = pl.pallas_call(
        functools.partial(kernel, n, nz),
        out_shape=(
            jax.ShapeDtypeStruct((slabs, narrow, rows * n), jnp.bfloat16),
            jax.ShapeDtypeStruct((slabs, width), jnp.float32),
            jax.ShapeDtypeStruct((router_rows * nz, rows * n), jnp.bfloat16),
        ),
        in_specs=[hbm, hbm, vmem, vmem],
        out_specs=(hbm, vmem, hbm),
        scratch_shapes=[
            pltpu.VMEM((slabs, rows, width), jnp.float32),
            pltpu.VMEM((SLOTS, width, rows), jnp.bfloat16),
            pltpu.VMEM((groups, GROUP, width), jnp.float32),
            pltpu.VMEM((groups, n - 1, GROUP, width), jnp.float32),
            pltpu.VMEM((width // LANES, slabs, LANES), jnp.float32),
            pltpu.VMEM((router_rows * nz, rows), jnp.bfloat16),
            dma((slabs,)), dma((SLOTS, n - 1)), dma((SLOTS,)), dma((n - 1,)),
            dma((groups, n - 1)), dma((groups, n - 1)),
            dma((nz - 1,)), dma((nz - 1,)), dma((n - 1,)), dma((n - 1,)), dma,
        ],
        compiler_params=pltpu.CompilerParams(
            collective_id=0, has_side_effects=True, vmem_limit_bytes=VMEM_LIMIT),
    )(master_gate, master_up, router_weight.T, router_gain[None, :])
    me = lax.axis_index("shard")
    scale = lax.dynamic_slice_in_dim(scale, me * narrow, narrow, axis=1)
    return (
        out[:experts].swapaxes(1, 2), out[experts:].swapaxes(1, 2),
        scale[:experts], scale[experts:], router.T,
    )


def solution(mesh):
    n, nz = mesh.shape["shard"], mesh.shape["expert"]

    def local(master_gate, master_up, router_weight, router_gain):
        experts, rows, width = master_gate.shape
        slabs = 2 * experts
        held = slabs * rows * width * 4 + SLOTS * rows * width * 2 + slabs * (n + 4) * width * 4
        fits = (
            n > 1 and nz > 1 and held <= VMEM_LIMIT and rows % LANES == 0 and width % LANES == 0
            and width % (16 * n) == 0 and slabs % GROUP == 0 and slabs >= 2 * GROUP
            and slabs > SLOTS and router_weight.shape[1] % 16 == 0
        )
        if not fits:
            return plain(master_gate, master_up, router_weight, router_gain)
        return fused(n, nz, master_gate, master_up, router_weight, router_gain)

    in_specs = (
        P("expert", "shard", None),
        P("expert", "shard", None),
        P("shard", "expert"),
        P("shard"),
    )
    out_specs = (
        P("expert", None, "shard"),
        P("expert", None, "shard"),
        P("expert", "shard"),
        P("expert", "shard"),
        P(),
    )
    return jax.shard_map(local, mesh=mesh, in_specs=in_specs, out_specs=out_specs, check_vma=False)
```

```python
import functools

import jax
import jax.numpy as jnp
from jax import lax
from jax.experimental import pallas as pl
from jax.experimental.pallas import tpu as pltpu
from jax.sharding import PartitionSpec as P

GROUP = 8
SLOTS = 16
LANES = 128
VMEM_LIMIT = 62914560


def plain(master_gate, master_up, router_weight, router_gain):
    total_gate, total_up = lax.psum(
        (jnp.sum(master_gate * master_gate, axis=1), jnp.sum(master_up * master_up, axis=1)),
        "shard",
    )
    scale_gate = jnp.sqrt(total_gate)
    scale_up = jnp.sqrt(total_up)
    narrow_gate, narrow_up = (
        (master_gate / jnp.expand_dims(scale_gate, 1)).astype(jnp.bfloat16),
        (master_up / jnp.expand_dims(scale_up, 1)).astype(jnp.bfloat16),
    )
    final_gate, final_up = (
        lax.all_to_all(narrow_gate, "shard", split_axis=2, concat_axis=1, tiled=True),
        lax.all_to_all(narrow_up, "shard", split_axis=2, concat_axis=1, tiled=True),
    )
    scale_gate = lax.dynamic_slice_in_dim(
        scale_gate, lax.axis_index("shard") * final_gate.shape[2], final_gate.shape[2], axis=1
    )
    scale_up = lax.dynamic_slice_in_dim(
        scale_up, lax.axis_index("shard") * final_up.shape[2], final_up.shape[2], axis=1
    )
    part_router = (router_weight * router_gain[:, None]).astype(jnp.bfloat16)
    row_router = lax.all_gather(part_router, "shard", axis=0, tiled=True)
    serve_router = lax.all_gather(row_router, "expert", axis=1, tiled=True)
    return (final_gate, final_up, scale_gate, scale_up, serve_router)


def kernel(n, nz, gate, up, weight, gain, out, scale_out, router_out,
           buf, slots, part, got, inverse, column,
           load_sem, send_sem, own_sem, recv_sem, part_send, part_recv,
           first_send, first_recv, second_send, second_recv, router_own):
    me = lax.axis_index("shard")
    mez = lax.axis_index("expert")
    experts, rows, width = gate.shape
    slabs = 2 * experts
    groups = slabs // GROUP
    narrow = width // n
    router_rows = weight.shape[0]

    def load(source, e, k):
        return pltpu.make_async_copy(source.at[e], buf.at[k], load_sem.at[k])

    def start_gate(e, _):
        load(gate, e, e).start()
        return 0

    def start_up(e, _):
        load(up, e, experts + e).start()
        return 0

    lax.fori_loop(0, experts, start_gate, 0)
    lax.fori_loop(0, experts, start_up, 0)

    barrier = pltpu.get_barrier_semaphore()
    for r in range(1, n):
        pl.semaphore_signal(barrier, inc=1, device_id={"shard": lax.rem(me + r, n)},
                            device_id_type=pl.DeviceIdType.MESH)
    for r in range(1, nz):
        pl.semaphore_signal(barrier, inc=1, device_id={"expert": lax.rem(mez + r, nz)},
                            device_id_type=pl.DeviceIdType.MESH)

    my_rows = pl.ds(pl.multiple_of(mez * router_rows, router_rows), router_rows)
    my_lanes = pl.ds(pl.multiple_of(me * rows, rows), rows)
    column[my_rows, :] = (weight[...] * gain[...]).astype(jnp.bfloat16)
    pl.semaphore_wait(barrier, n - 1 + nz - 1)

    def sums(g):
        def one(i, _):
            k = g * GROUP + i
            load(gate, 0, k).wait()
            x = buf[k]
            part[g, pl.ds(i, 1), :] = jnp.sum(x * x, axis=0, keepdims=True)

            if g == 1:
                @pl.when(i == 0)
                def _():
                    send_part(0)
            return 0
        lax.fori_loop(0, GROUP, one, 0)

    def part_copy(g, r):
        return pltpu.make_async_remote_copy(
            src_ref=part.at[g], dst_ref=got.at[g, r - 1],
            send_sem=part_send.at[g, r - 1], recv_sem=part_recv.at[g, r - 1],
            device_id={"shard": lax.rem(me + r, n)}, device_id_type=pl.DeviceIdType.MESH)

    def send_part(g):
        for r in range(1, n):
            part_copy(g, r).start()

    def first_copy(r):
        return pltpu.make_async_remote_copy(
            src_ref=column.at[my_rows, :], dst_ref=column.at[my_rows, :],
            send_sem=first_send.at[r - 1], recv_sem=first_recv.at[r - 1],
            device_id={"expert": lax.rem(mez + r, nz)}, device_id_type=pl.DeviceIdType.MESH)

    def second_copy(r):
        return pltpu.make_async_remote_copy(
            src_ref=column, dst_ref=router_out.at[:, my_lanes],
            send_sem=second_send.at[r - 1], recv_sem=second_recv.at[r - 1],
            device_id={"shard": lax.rem(me + r, n)}, device_id_type=pl.DeviceIdType.MESH)

    own_router = pltpu.make_async_copy(column, router_out.at[:, my_lanes], router_own)

    def slab_copy(k, r):
        target = lax.rem(me + r, n)
        s = k % SLOTS
        return pltpu.make_async_remote_copy(
            src_ref=slots.at[s, pl.ds(pl.multiple_of(target * narrow, 16), narrow), :],
            dst_ref=out.at[k, :, my_lanes],
            send_sem=send_sem.at[s, r - 1], recv_sem=recv_sem.at[r - 1],
            device_id={"shard": target}, device_id_type=pl.DeviceIdType.MESH)

    def own_copy(k):
        s = k % SLOTS
        return pltpu.make_async_copy(
            slots.at[s, pl.ds(pl.multiple_of(me * narrow, 16), narrow), :],
            out.at[k, :, my_lanes], own_sem.at[s])

    def send_slab(k):
        for r in range(1, n):
            slab_copy(k, r).start()
        own_copy(k).start()

    def wait_slab(k):
        for r in range(1, n):
            slab_copy(k, r).wait_send()
        own_copy(k).wait()

    def narrow_slab(g, i):
        k = g * GROUP + i

        @pl.when(k >= SLOTS)
        def _():
            wait_slab(k - SLOTS)

        s = k % SLOTS

        def tile(j, _):
            lanes = pl.ds(pl.multiple_of(j * LANES, LANES), LANES)
            y = buf[k, :, lanes] * inverse[j, pl.ds(k, 1), :]
            slots[s, lanes, :] = y.T.astype(jnp.bfloat16)
            return 0

        lax.fori_loop(0, width // LANES, tile, 0)

    sums(0)
    for r in range(1, nz):
        first_copy(r).start()
    sums(1)

    for g in range(groups):
        for r in range(1, n):
            part_copy(g, r).wait_recv()
        total = part[g]
        for r in range(1, n):
            total = total + got[g, r - 1]
        scale = jnp.sqrt(total)
        scale_out[g * GROUP:(g + 1) * GROUP, :] = scale
        reciprocal = 1.0 / scale
        for j in range(width // LANES):
            inverse[j, g * GROUP:(g + 1) * GROUP, :] = reciprocal[:, j * LANES:(j + 1) * LANES]

        def step(i, _):
            narrow_slab(g, i)
            k = g * GROUP + i

            @pl.when(k > 0)
            def _():
                send_slab(k - 1)

            if g == 0:
                @pl.when(k == 0)
                def _():
                    send_part(1)
            return 0

        lax.fori_loop(0, GROUP, step, 0)

        if g == 0:
            for r in range(1, nz):
                first_copy(r).wait()
            for later in range(2, groups):
                sums(later)
                if later > 2:
                    send_part(later - 1)
            for r in range(1, n):
                second_copy(r).start()
            own_router.start()
            if groups > 2:
                send_part(groups - 1)

    for r in range(1, n):
        second_copy(r).wait_send()
    for g in range(groups):
        for r in range(1, n):
            part_copy(g, r).wait_send()
    send_slab(slabs - 1)

    def drain(k, _):
        wait_slab(k)
        return 0

    lax.fori_loop(max(slabs - SLOTS, 0), slabs, drain, 0)
    own_router.wait()
    for r in range(1, n):
        second_copy(r).wait_recv()
        whole = out.at[:, :, my_lanes]
        pltpu.make_async_remote_copy(
            src_ref=whole, dst_ref=whole,
            send_sem=send_sem.at[0, r - 1], recv_sem=recv_sem.at[r - 1],
            device_id={"shard": lax.rem(me + r, n)}, device_id_type=pl.DeviceIdType.MESH,
        ).wait_recv()


def fused(n, nz, master_gate, master_up, router_weight, router_gain):
    experts, rows, width = master_gate.shape
    slabs = 2 * experts
    groups = slabs // GROUP
    narrow = width // n
    router_rows = router_weight.shape[1]
    hbm = pl.BlockSpec(memory_space=pl.ANY)
    vmem = pl.BlockSpec(memory_space=pltpu.VMEM)
    dma = pltpu.SemaphoreType.DMA
    out, scale, router = pl.pallas_call(
        functools.partial(kernel, n, nz),
        out_shape=(
            jax.ShapeDtypeStruct((slabs, narrow, rows * n), jnp.bfloat16),
            jax.ShapeDtypeStruct((slabs, width), jnp.float32),
            jax.ShapeDtypeStruct((router_rows * nz, rows * n), jnp.bfloat16),
        ),
        in_specs=[hbm, hbm, vmem, vmem],
        out_specs=(hbm, vmem, hbm),
        scratch_shapes=[
            pltpu.VMEM((slabs, rows, width), jnp.float32),
            pltpu.VMEM((SLOTS, width, rows), jnp.bfloat16),
            pltpu.VMEM((groups, GROUP, width), jnp.float32),
            pltpu.VMEM((groups, n - 1, GROUP, width), jnp.float32),
            pltpu.VMEM((width // LANES, slabs, LANES), jnp.float32),
            pltpu.VMEM((router_rows * nz, rows), jnp.bfloat16),
            dma((slabs,)), dma((SLOTS, n - 1)), dma((SLOTS,)), dma((n - 1,)),
            dma((groups, n - 1)), dma((groups, n - 1)),
            dma((nz - 1,)), dma((nz - 1,)), dma((n - 1,)), dma((n - 1,)), dma,
        ],
        compiler_params=pltpu.CompilerParams(
            collective_id=0, has_side_effects=True, vmem_limit_bytes=VMEM_LIMIT),
    )(master_gate, master_up, router_weight.T, router_gain[None, :])
    me = lax.axis_index("shard")
    scale = lax.dynamic_slice_in_dim(scale, me * narrow, narrow, axis=1)
    return (
        out[:experts].swapaxes(1, 2), out[experts:].swapaxes(1, 2),
        scale[:experts], scale[experts:], router.T,
    )


def solution(mesh):
    n, nz = mesh.shape["shard"], mesh.shape["expert"]

    def local(master_gate, master_up, router_weight, router_gain):
        experts, rows, width = master_gate.shape
        slabs = 2 * experts
        held = slabs * rows * width * 4 + SLOTS * rows * width * 2 + slabs * (n + 4) * width * 4
        fits = (
            n > 1 and nz > 1 and held <= VMEM_LIMIT and rows % LANES == 0 and width % LANES == 0
            and width % (16 * n) == 0 and slabs % GROUP == 0 and slabs >= 2 * GROUP
            and slabs > SLOTS and router_weight.shape[1] % 16 == 0
        )
        if not fits:
            return plain(master_gate, master_up, router_weight, router_gain)
        return fused(n, nz, master_gate, master_up, router_weight, router_gain)

    in_specs = (
        P("expert", "shard", None),
        P("expert", "shard", None),
        P("shard", "expert"),
        P("shard"),
    )
    out_specs = (
        P("expert", None, "shard"),
        P("expert", None, "shard"),
        P("expert", "shard"),
        P("expert", "shard"),
        P(),
    )
    return jax.shard_map(local, mesh=mesh, in_specs=in_specs, out_specs=out_specs, check_vma=False)
```
